32 devices in a mesh: grp: 4 (over x, core), dev: 8 (over z, y).
Axes of the slice: x: 2, y: 2, z: 4, core: 2. Of those that a mesh axis runs over, the one named last changes fastest.
Arguments:
- node_features: float32 [16384, 768], P(('grp', 'dev')), may hold values from -6 to 6
- tiles: bfloat16 [896, 128, 128], P(('grp', 'dev')), may hold values from -0.1875 to 0.1875
- tile_list: int32 [896, 2], replicated, may hold values from 0 to 127, as said below
- weight: float32 [768, 768], replicated, may hold values from -0.21875 to 0.21875
- texts: float32 [1024, 768], P(('grp', 'dev')), may hold values from -6 to 6
- selected: int32 [1024], P(('grp', 'dev')), may hold values from 0 to 16383, as said below
- pairing: int32 [1024], P(('grp', 'dev')), may hold values from 0 to 1023, each once
Outputs:
- contrast_loss: float32 [], replicated
- grad_nodes: float32 [16384, 768], P(('grp', 'dev'))
- grad_weight: float32 [768, 768], replicated
- grad_texts: float32 [1024, 768], P(('grp', 'dev'))
The draws below stay inside these ranges and needn't reach their ends.
Inputs may be any that keep to these rules, and one draw needn't show every extreme that they name: `tile_list`: device number p = grp index * (devices along dev) + dev index holds node blocks p * 4 to (p + 1) * 4 - 1 and tiles p * 28 to (p + 1) * 28 - 1. A tile's row block lies on the device that holds the tile; its column block lies on that device, on another device of the same grp index, or on the device of the same dev index in another grp. At most 2 tiles of one device have column blocks on any one other device; in every draw each device has one other device of its grp index and one of its dev index at that most. `selected`: distinct ids; the ids listed on a device are nodes of that device.
All inputs are finite; a program needn't handle non-finite values.
Results may differ from the reference program's by a relative error of at most 0.0004.
The reference program's roundings to bfloat16 on the way (of `rounded` and `rounded_grads`) count: a program that leaves them out, or rounds other values in their place, can miss the bound.
Values may be sent and summed in bfloat16 or wider, within the bound.
No kernel may reach another device: no remote copies, remote signals or barrier semaphores. Data moves between devices by JAX's collectives and lax.ppermute only.
A program may use at most 128 MiB of HBM per device.

```python
import jax
import jax.numpy as jnp
from jax import lax

D = 768
BLOCK = 128
NB_DEV = 4
CAP = 2
SEL_DEV = 32
TILE_DEV = 28
NODES = 16384
TILES = 896
SEL = 1024
N_GRP = 4
N_DEV = 8


def draw_tile_list(key, part):
    pool_dev = CAP * (N_DEV - 1)
    pool_all = pool_dev + CAP * (N_GRP - 1)

    def one_device(device):
        sub_key = jax.random.fold_in(jax.random.fold_in(key, 7151), device)
        keys = jax.random.split(sub_key, 7)
        grp_index = device // N_DEV
        dev_index = device % N_DEV
        entries = jnp.arange(pool_all, dtype=jnp.int32)
        is_dev = entries < pool_dev
        near_pick = entries // CAP
        far_pick = (entries - pool_dev) // CAP
        peer_dev = near_pick + (near_pick >= dev_index).astype(jnp.int32)
        peer_grp = far_pick + (far_pick >= grp_index).astype(jnp.int32)
        peer = jnp.where(is_dev, grp_index * N_DEV + peer_dev, peer_grp * N_DEV + dev_index)
        forced_dev = jax.random.randint(keys[0], (), 0, N_DEV - 1)
        forced_grp = jax.random.randint(keys[1], (), 0, N_GRP - 1)
        forced = is_dev & (near_pick == forced_dev) | jnp.logical_not(is_dev) & (far_pick == forced_grp)
        priority = jax.random.permutation(keys[2], pool_all).astype(jnp.int32) + pool_all * forced.astype(jnp.int32)
        order_list = jnp.argsort(-priority)
        chosen_peers = peer[order_list]
        lowest = max(pool_all // 2, 2 * CAP)
        count = jax.random.randint(keys[3], (), lowest, pool_all + 1)
        slots = jnp.arange(TILE_DEV, dtype=jnp.int32)
        col_owner = jnp.where(slots < count, chosen_peers[jnp.minimum(slots, pool_all - 1)], device)
        col_owner = col_owner[jax.random.permutation(keys[4], TILE_DEV)]
        col_block = col_owner * NB_DEV + jax.random.randint(keys[5], (TILE_DEV,), 0, NB_DEV)
        row_block = device * NB_DEV + jax.random.randint(keys[6], (TILE_DEV,), 0, NB_DEV)
        return jnp.stack([row_block, col_block], axis=1).astype(jnp.int32)
    listed = jax.vmap(one_device)(jnp.arange(N_GRP * N_DEV, dtype=jnp.int32))
    return listed.reshape(TILES, 2).astype(jnp.int32)


def draw_selected(key, part):

    def one_device(device):
        sub_key = jax.random.fold_in(jax.random.fold_in(key, 9203), device)
        order_list = jax.random.permutation(sub_key, NB_DEV * BLOCK).astype(jnp.int32)
        return order_list[:SEL_DEV] + device * NB_DEV * BLOCK
    listed = jax.vmap(one_device)(jnp.arange(N_GRP * N_DEV, dtype=jnp.int32))
    return listed.reshape(SEL).astype(jnp.int32)


def shard_levels(own_key, dims, pieces, least, high):
    gain = 1.0
    for dim, parts in pieces:
        draws = jax.random.uniform(jax.random.fold_in(jax.random.fold_in(own_key, 6), dim), (parts,), jnp.float32, least / len(pieces), high / len(pieces))
        gain = gain * jnp.repeat(jnp.exp(draws), dims[dim] // parts).reshape((-1,) + (1,) * (len(dims) - 1 - dim))
    return gain


def bell_draw(key, extent, width, bound, cuts=(), kind=jnp.bfloat16):
    result = width * jax.random.normal(key, extent, jnp.float32)
    if cuts:
        result = result * shard_levels(key, extent, cuts, -0.22, 0.18)
    return jnp.clip(result, -bound, bound).astype(kind)


def setup_inputs(seed: int = 0) -> dict:
    streams_of = jax.random.split(jax.random.key(seed), 8)
    node_features = bell_draw(streams_of[0], (NODES, D), 1.0, 6.0, ((0, 32),), jnp.float32)
    tiles = bell_draw(streams_of[1], (TILES, BLOCK, BLOCK), (BLOCK * TILE_DEV // NB_DEV) ** -0.5, 0.1875, ((0, 32),))
    tile_list = draw_tile_list(jax.random.fold_in(streams_of[7], 71), 0)
    weight = bell_draw(streams_of[3], (D, D), D ** -0.5, 0.21875, (), jnp.float32)
    texts = bell_draw(streams_of[4], (SEL, D), 1.0, 6.0, ((0, 32),), jnp.float32)
    selected = draw_selected(jax.random.fold_in(streams_of[7], 71), 0)
    pairing = jax.random.permutation(streams_of[6], SEL).astype(jnp.int32)
    return dict(node_features=node_features, tiles=tiles, tile_list=tile_list, weight=weight, texts=texts, selected=selected, pairing=pairing)


SCALE = 1.0 / 0.07
EPS = 1e-06
PRECISE = lax.Precision.HIGHEST
ROOT_HALF = 0.7071067811865476
INV_ROOT_TWO_PI = 0.3989422804014327

def gelu_value(value):
    return 0.5 * value * (1.0 + lax.erf(value * ROOT_HALF))

def gelu_slope(value):
    return 0.5 * (1.0 + lax.erf(value * ROOT_HALF)) + value * jnp.exp(-0.5 * value * value) * INV_ROOT_TWO_PI

def reference(node_features, tiles, tile_list, weight, texts, selected, pairing):
    blocks_all = NODES // BLOCK
    rounded = lax.optimization_barrier(node_features.astype(jnp.bfloat16))
    source = rounded.astype(jnp.float32).reshape(blocks_all, BLOCK, D)
    row_blocks = tile_list[:, 0]
    col_blocks = tile_list[:, 1]

    def forward_step(total, device):
        start = (device * TILE_DEV).astype(jnp.int32)
        matrices = lax.dynamic_slice_in_dim(tiles, start, TILE_DEV, 0).astype(jnp.float32)
        rows_here = lax.dynamic_slice_in_dim(row_blocks, start, TILE_DEV, 0)
        cols_here = lax.dynamic_slice_in_dim(col_blocks, start, TILE_DEV, 0)
        products = jnp.einsum('tij,tjd->tid', matrices, source[cols_here], precision=PRECISE)
        return (total.at[rows_here].add(products), None)
    devices_all = jnp.arange(N_GRP * N_DEV, dtype=jnp.int32)
    messages, _ = lax.scan(forward_step, jnp.zeros((blocks_all, BLOCK, D), jnp.float32), devices_all)
    mixed = node_features + messages.reshape(NODES, D)
    chosen = mixed[selected]
    before = jnp.dot(chosen, weight, precision=PRECISE)
    hidden = gelu_value(before)
    node_norm = jnp.sqrt(lax.optimization_barrier(jnp.sum(hidden * hidden, axis=1, keepdims=True)) + EPS)
    unit_nodes = hidden / node_norm
    text_norm = jnp.sqrt(lax.optimization_barrier(jnp.sum(texts * texts, axis=1, keepdims=True)) + EPS)
    unit_texts = texts / text_norm
    scores = SCALE * jnp.dot(unit_nodes, unit_texts.T, precision=PRECISE)
    row_lse = jnp.log(lax.optimization_barrier(jnp.sum(jnp.exp(scores), axis=1)))
    col_lse = jnp.log(lax.optimization_barrier(jnp.sum(jnp.exp(scores), axis=0)))
    target = pairing[:, None] == jnp.arange(SEL, dtype=jnp.int32)[None, :]
    positive = jnp.sum(jnp.where(target, scores, jnp.zeros_like(scores)))
    contrast_loss = (jnp.sum(row_lse) + jnp.sum(col_lse)) / (2.0 * SEL) - positive / SEL
    score_grads = 0.5 * (jnp.exp(scores - row_lse[:, None]) + jnp.exp(scores - col_lse[None, :])) - target.astype(jnp.float32)
    node_dir = SCALE * jnp.dot(score_grads, unit_texts, precision=PRECISE)
    text_dir = SCALE * jnp.dot(score_grads.T, unit_nodes, precision=PRECISE)
    node_back = (node_dir - unit_nodes * lax.optimization_barrier(jnp.sum(unit_nodes * node_dir, axis=1, keepdims=True))) / node_norm
    grad_texts = (text_dir - unit_texts * lax.optimization_barrier(jnp.sum(unit_texts * text_dir, axis=1, keepdims=True))) / text_norm
    pre_grad = node_back * gelu_slope(before)
    grad_weight = jnp.dot(chosen.T, pre_grad, precision=PRECISE)
    row_grads = jnp.dot(pre_grad, weight.T, precision=PRECISE)
    dense_grads = jnp.zeros((NODES, D), jnp.float32).at[selected].add(row_grads)
    rounded_grads = lax.optimization_barrier(dense_grads.astype(jnp.bfloat16))
    grad_source = rounded_grads.astype(jnp.float32).reshape(blocks_all, BLOCK, D)

    def backward_step(total, device):
        start = (device * TILE_DEV).astype(jnp.int32)
        matrices = lax.dynamic_slice_in_dim(tiles, start, TILE_DEV, 0).astype(jnp.float32)
        rows_here = lax.dynamic_slice_in_dim(row_blocks, start, TILE_DEV, 0)
        cols_here = lax.dynamic_slice_in_dim(col_blocks, start, TILE_DEV, 0)
        products = jnp.einsum('tij,tid->tjd', matrices, grad_source[rows_here], precision=PRECISE)
        return (total.at[cols_here].add(products), None)
    back_terms, _ = lax.scan(backward_step, jnp.zeros((blocks_all, BLOCK, D), jnp.float32), devices_all)
    grad_nodes = dense_grads + back_terms.reshape(NODES, D)
    return (contrast_loss, grad_nodes, grad_weight, grad_texts)
```

```python
import functools

import jax
import jax.numpy as jnp
from jax import lax
from jax.experimental import pallas as pl
from jax.experimental.pallas import tpu as pltpu
from jax.sharding import PartitionSpec as P

CAP = 2


SCALE = 1.0 / 0.07
EPS = 1e-06
PRECISE = lax.Precision.HIGHEST
ROOT_HALF = 0.7071067811865476
INV_ROOT_TWO_PI = 0.3989422804014327
VMEM_SPEC = pl.BlockSpec(memory_space=pltpu.VMEM)
SMEM_SPEC = pl.BlockSpec(memory_space=pltpu.SMEM)


def gelu_value(value):
    return 0.5 * value * (1.0 + lax.erf(value * ROOT_HALF))


def gelu_slope(value):
    return (
        0.5 * (1.0 + lax.erf(value * ROOT_HALF))
        + value * jnp.exp(-0.5 * value * value) * INV_ROOT_TWO_PI
    )


def place():
    members = lax.axis_size("dev")
    return lax.axis_index("grp"), lax.axis_index("dev"), members


def pick_kernel(blocks_dev, flat, sel, pair, tiles, near, far, rows, selm, count, where_to):
    grp, dev, members = place()
    device = grp * members + dev
    tile_dev, block_rows, _ = tiles.shape
    sel_dev = selm.shape[0]
    base = device * blocks_dev * block_rows
    lane = lax.broadcasted_iota(jnp.int32, (1, block_rows), 1)
    coded = jnp.zeros((1, block_rows), jnp.int32)
    for k in range(sel_dev):
        selm[k : k + 1, :] = (sel[k] - base) - lane
        coded = jnp.where(lane == k, pair[k], coded)
    near[...] = jnp.zeros_like(near)
    far[...] = jnp.zeros_like(far)
    for i in range(count.shape[0]):
        count[i] = 0
    offsets = selm[...]
    for t in range(tile_dev):
        row_block = flat[2 * (device * tile_dev + t)] - device * blocks_dev
        hot = (offsets == row_block * block_rows).astype(jnp.bfloat16)
        rows[t] = jnp.dot(hot, tiles[t], preferred_element_type=jnp.float32).astype(jnp.bfloat16)
    high = coded // block_rows
    high_row = high.astype(jnp.float32).astype(jnp.bfloat16)
    low_row = (coded - high * block_rows).astype(jnp.float32).astype(jnp.bfloat16)
    for q in range(near.shape[0]):
        near[q, CAP, 0:1, :] = high_row
        near[q, CAP, 1:2, :] = low_row

    def step(t, carry):
        owner = flat[2 * (device * tile_dev + t) + 1] // blocks_dev
        rank = count[owner]
        count[owner] = rank + 1
        owner_grp = owner // members
        owner_dev = owner - owner_grp * members

        @pl.when((owner_grp == grp) & (owner_dev != dev))
        def _():
            near[owner_dev, rank] = rows[t]

        @pl.when(owner_grp != grp)
        def _():
            far[owner_grp, rank] = rows[t]

        return carry

    lax.fori_loop(0, tile_dev, step, 0)


def local_kernel(flat, sel, feats, rows, blocks, local, index):
    grp, dev, members = place()
    groups = lax.axis_size("grp")
    device = grp * members + dev
    blocks_dev, block_rows, _ = blocks.shape
    tile_dev, sel_dev, _ = rows.shape
    base = device * blocks_dev * block_rows
    for c in range(blocks_dev):
        blocks[c] = feats[c * block_rows : (c + 1) * block_rows, :].astype(jnp.bfloat16)
    for k in range(sel_dev):
        local[k : k + 1, :] = feats[pl.ds(sel[k] - base, 1), :]

    def add_tile(t, carry):
        column = flat[2 * (device * tile_dev + t) + 1]

        @pl.when(column // blocks_dev == device)
        def _():
            local[...] += jnp.dot(
                rows[t], blocks[column - device * blocks_dev], preferred_element_type=jnp.float32
            )

        return carry

    lax.fori_loop(0, tile_dev, add_tile, 0)
    for i in range(index.shape[0]):
        index[i] = 0
    for q in range(members + groups):
        peer = grp * members + q if q < members else (q - members) * members + dev

        def scan(t, hits, q=q, peer=peer):
            column = flat[2 * (peer * tile_dev + t) + 1]
            mine = column // blocks_dev == device
            index[q * (CAP + 1) + hits] = jnp.clip(column - device * blocks_dev, 0, blocks_dev - 1)
            return jnp.minimum(hits + mine.astype(jnp.int32), CAP)

        lax.fori_loop(0, tile_dev, scan, 0)


def partial_kernel(index, near_in, far_in, blocks, local, near_part, far_part):
    _, dev, members = place()
    groups = far_in.shape[0]
    for q in range(members + groups):
        source = near_in if q < members else far_in
        target = near_part if q < members else far_part
        p = q if q < members else q - members
        total = jnp.dot(
            source[p, 0], blocks[index[q * (CAP + 1)]], preferred_element_type=jnp.float32
        )
        for s in range(1, CAP):
            total += jnp.dot(
                source[p, s], blocks[index[q * (CAP + 1) + s]], preferred_element_type=jnp.float32
            )
        target[p] = total
    near_part[dev] = local[...]


def spread_kernel(
    blocks_dev, flat, sel, index, near_in, far_in, rows, near_grads, far_grads, row_grads, out
):
    grp, dev, members = place()
    device = grp * members + dev
    groups = far_in.shape[0]
    tile_dev, sel_dev, block_rows = rows.shape
    base = device * blocks_dev * block_rows
    across = (((0,), (0,)), ((), ()))
    out[...] = jnp.zeros_like(out)
    for q in range(members + groups):
        source = near_in if q < members else far_in
        grads = near_grads if q < members else far_grads
        p = q if q < members else q - members
        for s in range(CAP):
            c = index[q * (CAP + 1) + s]
            span = pl.ds(pl.multiple_of(c * block_rows, block_rows), block_rows)
            out[span, :] += lax.dot_general(
                source[p, s], grads[p], across, preferred_element_type=jnp.float32
            )
    own = near_grads[dev]

    def add_tile(t, carry):
        column = flat[2 * (device * tile_dev + t) + 1]

        @pl.when(column // blocks_dev == device)
        def _():
            c = column - device * blocks_dev
            span = pl.ds(pl.multiple_of(c * block_rows, block_rows), block_rows)
            out[span, :] += lax.dot_general(
                rows[t], own, across, preferred_element_type=jnp.float32
            )

        return carry

    lax.fori_loop(0, tile_dev, add_tile, 0)
    for k in range(sel_dev):
        out[pl.ds(sel[k] - base, 1), :] += row_grads[k : k + 1, :]


def split_size(count):
    return next(n for n in (4, 2, 1) if count % n == 0)


def gather_axis(part, axis, outer, inner, outer_first=True):
    def shift(value, do, di):
        pairs = [
            (((o + do) % outer) * inner + (i + di) % inner, o * inner + i)
            for o in range(outer)
            for i in range(inner)
        ]
        return lax.ppermute(value, axis, pairs)

    stage = jnp.stack([part] + [shift(part, j, 0) for j in range(1, outer)])
    return jnp.stack([stage] + [shift(stage, 0, j) for j in range(1, inner)])


def offsets(index, outer, inner):
    o = (index // inner + jnp.arange(outer, dtype=jnp.int32)) % outer
    i = (index % inner + jnp.arange(inner, dtype=jnp.int32)) % inner
    return o[None, :] * inner + i[:, None]


def shards(node_features, tiles, tile_list, weight, texts, selected, pairing):
    groups = lax.axis_size("grp")
    members = lax.axis_size("dev")
    grp_index = lax.axis_index("grp")
    dev_index = lax.axis_index("dev")
    block_rows = tiles.shape[1]
    feat_width = node_features.shape[1]
    blocks_dev = node_features.shape[0] // block_rows
    tile_dev = tiles.shape[0]
    sel_dev = selected.shape[0]
    total_sel = sel_dev * groups * members
    group_sel = sel_dev * members
    f32 = jnp.float32
    grp_inner = 2 if groups % 2 == 0 else 1
    grp_outer = groups // grp_inner
    dev_outer = split_size(members)
    dev_inner = members // dev_outer
    flat = tile_list.reshape(-1)

    near_rows, far_rows, tile_rows = pl.pallas_call(
        functools.partial(pick_kernel, blocks_dev),
        out_shape=(
            jax.ShapeDtypeStruct((members, CAP + 1, sel_dev, block_rows), jnp.bfloat16),
            jax.ShapeDtypeStruct((groups, CAP, sel_dev, block_rows), jnp.bfloat16),
            jax.ShapeDtypeStruct((tile_dev, sel_dev, block_rows), jnp.bfloat16),
        ),
        in_specs=[SMEM_SPEC, SMEM_SPEC, SMEM_SPEC, VMEM_SPEC],
        out_specs=(VMEM_SPEC, VMEM_SPEC, VMEM_SPEC),
        scratch_shapes=[
            pltpu.VMEM((sel_dev, block_rows), jnp.int32),
            pltpu.SMEM((groups * members,), jnp.int32),
            pltpu.SMEM((8,), jnp.int32),
        ],
        cost_estimate=pl.CostEstimate(flops=2 * 10**6, bytes_accessed=10**6, transcendentals=0),
        name="pick",
    )(flat, selected, pairing, tiles)
    near_in = lax.all_to_all(near_rows, "dev", 0, 0, tiled=True)
    far_in = lax.all_to_all(far_rows, "grp", 0, 0, tiled=True)

    text_norm = jnp.sqrt(jnp.sum(texts * texts, axis=1, keepdims=True) + EPS)
    unit_texts = texts / text_norm
    text_near = gather_axis(unit_texts, "dev", dev_outer, dev_inner).reshape(group_sel, feat_width)
    text_all = gather_axis(text_near, "grp", grp_outer, grp_inner).reshape(total_sel, feat_width)
    grp_of = offsets(grp_index, grp_outer, grp_inner).reshape(-1)
    dev_of = offsets(dev_index, dev_outer, dev_inner).reshape(-1)
    text_id = (
        (grp_of[:, None, None] * members + dev_of[None, :, None]) * sel_dev
        + jnp.arange(sel_dev, dtype=jnp.int32)[None, None, :]
    ).reshape(-1)

    blocks, local, index = pl.pallas_call(
        local_kernel,
        out_shape=(
            jax.ShapeDtypeStruct((blocks_dev, block_rows, feat_width), jnp.bfloat16),
            jax.ShapeDtypeStruct((sel_dev, feat_width), f32),
            jax.ShapeDtypeStruct(((members + groups) * (CAP + 1),), jnp.int32),
        ),
        in_specs=[SMEM_SPEC, SMEM_SPEC, VMEM_SPEC, VMEM_SPEC],
        out_specs=(VMEM_SPEC, VMEM_SPEC, SMEM_SPEC),
        cost_estimate=pl.CostEstimate(flops=2 * 10**6, bytes_accessed=10**6, transcendentals=0),
        name="local",
    )(flat, selected, node_features, tile_rows)
    near_part, far_part = pl.pallas_call(
        partial_kernel,
        out_shape=(
            jax.ShapeDtypeStruct((members, sel_dev, feat_width), f32),
            jax.ShapeDtypeStruct((groups, sel_dev, feat_width), f32),
        ),
        in_specs=[SMEM_SPEC, VMEM_SPEC, VMEM_SPEC, VMEM_SPEC, VMEM_SPEC],
        out_specs=(VMEM_SPEC, VMEM_SPEC),
        cost_estimate=pl.CostEstimate(flops=2 * 10**6, bytes_accessed=10**6, transcendentals=0),
        name="partial",
    )(index, near_in, far_in, blocks, local)
    near_back = lax.all_to_all(near_part, "dev", 0, 0, tiled=True)
    far_back = lax.all_to_all(far_part, "grp", 0, 0, tiled=True)
    own_chosen = jnp.sum(near_back, axis=0) + jnp.sum(far_back, axis=0)

    chosen = lax.all_to_all(
        jnp.broadcast_to(own_chosen[None], (members, sel_dev, feat_width)), "dev", 0, 0, tiled=True
    ).reshape(group_sel, feat_width)
    chosen_all = gather_axis(chosen, "grp", grp_outer, grp_inner).reshape(total_sel, feat_width)
    coded = near_in[:, CAP, :2, :sel_dev].astype(jnp.int32)
    pair_rows = (coded[:, 0, :] * block_rows + coded[:, 1, :]).reshape(-1)

    before = jnp.dot(chosen, weight, precision=PRECISE)
    hidden = gelu_value(before)
    node_norm = jnp.sqrt(jnp.sum(hidden * hidden, axis=1, keepdims=True) + EPS)
    unit_nodes = hidden / node_norm
    scores = SCALE * lax.dot_general(
        unit_nodes, text_all, (((1,), (1,)), ((), ())), precision=PRECISE
    )
    target = pair_rows[:, None] == text_id[None, :]
    exp_scores = jnp.exp(scores)
    row_total = jnp.sum(exp_scores, axis=1)
    positive = jnp.sum(jnp.where(target, scores, 0.0))
    col_part = jnp.sum(exp_scores, axis=0).reshape(groups, group_sel)
    is_grp = grp_of[:, None] == jnp.arange(groups, dtype=jnp.int32)[None, :]
    col_ordered = jnp.sum(jnp.where(is_grp[:, :, None], col_part[:, None, :], 0.0), axis=0)
    lane = jnp.arange(group_sel, dtype=jnp.int32)
    sums = jnp.where(
        lane == 0, jnp.sum(jnp.log(row_total)), jnp.where(lane == 1, positive, 0.0)
    )
    totals = lax.psum(jnp.concatenate([col_ordered, sums[None, :]], axis=0), "grp")
    col_total = jnp.sum(
        jnp.where(is_grp[:, :, None], totals[None, :groups, :], 0.0), axis=1
    ).reshape(-1)
    contrast_loss = (totals[groups, 0] + jnp.sum(jnp.log(col_total))) / (
        2.0 * total_sel
    ) - totals[groups, 1] / total_sel

    score_grads = 0.5 * (
        exp_scores / row_total[:, None] + exp_scores / col_total[None, :]
    ) - target.astype(f32)
    node_dir = SCALE * jnp.dot(score_grads, text_all, precision=PRECISE)
    node_back = (
        node_dir - unit_nodes * jnp.sum(unit_nodes * node_dir, axis=1, keepdims=True)
    ) / node_norm
    pre_grad = node_back * gelu_slope(before)
    pre_all = gather_axis(pre_grad, "grp", grp_outer, grp_inner).reshape(total_sel, feat_width)
    row_grads = lax.dot_general(pre_grad, weight, (((1,), (1,)), ((), ())), precision=PRECISE)
    near_grads = row_grads.astype(jnp.bfloat16).reshape(members, sel_dev, feat_width)
    own_grads = lax.dynamic_index_in_dim(
        row_grads.reshape(members, sel_dev, feat_width), dev_index, 0, False
    )
    far_grads = lax.all_gather(own_grads.astype(jnp.bfloat16), "grp", axis=0)
    grad_nodes = pl.pallas_call(
        functools.partial(spread_kernel, blocks_dev),
        out_shape=jax.ShapeDtypeStruct(node_features.shape, f32),
        in_specs=[SMEM_SPEC] * 3 + [VMEM_SPEC] * 6,
        out_specs=VMEM_SPEC,
        cost_estimate=pl.CostEstimate(flops=2 * 10**6, bytes_accessed=10**6, transcendentals=0),
        name="spread",
    )(flat, selected, index, near_in, far_in, tile_rows, near_grads, far_grads, own_grads)

    own_cols = score_grads.reshape(group_sel, groups, members, sel_dev)[:, :, 0, :]
    text_part = SCALE * lax.dot_general(
        own_cols.reshape(group_sel, groups * sel_dev),
        unit_nodes,
        (((0,), (0,)), ((), ())),
        precision=PRECISE,
    ).reshape(groups, sel_dev, feat_width)
    text_dir = text_part[0]
    for r in range(1, groups):
        di, do = r // grp_outer, r % grp_outer
        pairs = [
            (o * grp_inner + i, ((o + do) % grp_outer) * grp_inner + (i + di) % grp_inner)
            for o in range(grp_outer)
            for i in range(grp_inner)
        ]
        text_dir = text_dir + lax.ppermute(text_part[r], "grp", pairs)
    grad_texts = (
        text_dir - unit_texts * jnp.sum(unit_texts * text_dir, axis=1, keepdims=True)
    ) / text_norm

    grad_weight = lax.dot_general(
        chosen_all, pre_all, (((0,), (0,)), ((), ())), precision=PRECISE
    )
    return (contrast_loss, grad_nodes, grad_weight, grad_texts)


def solution(mesh):
    return jax.shard_map(
        shards,
        mesh=mesh,
        in_specs=(
            P(("grp", "dev"), None),
            P(("grp", "dev"), None, None),
            P(),
            P(),
            P(("grp", "dev"), None),
            P(("grp", "dev")),
            P(("grp", "dev")),
        ),
        out_specs=(P(), P(("grp", "dev"), None), P(), P(("grp", "dev"), None)),
        check_vma=False,
    )
```

```python
import functools

import jax
import jax.numpy as jnp
from jax import lax
from jax.experimental import pallas as pl
from jax.experimental.pallas import tpu as pltpu
from jax.sharding import PartitionSpec as P

CAP = 2


SCALE = 1.0 / 0.07
EPS = 1e-06
ROOT_HALF = 0.7071067811865476
INV_ROOT_TWO_PI = 0.3989422804014327
VMEM_SPEC = pl.BlockSpec(memory_space=pltpu.VMEM)
SMEM_SPEC = pl.BlockSpec(memory_space=pltpu.SMEM)
PLAIN = (((1,), (0,)), ((), ()))
BY_LAST = (((1,), (1,)), ((), ()))
BY_FIRST = (((0,), (0,)), ((), ()))


def factors():
    groups = lax.axis_size("grp")
    inner = 2 if groups % 2 == 0 else 1
    return groups // inner, inner


def dev_factors():
    members = lax.axis_size("dev")
    outer = next(n for n in (4, 2, 1) if members % n == 0)
    return outer, members // outer


def place():
    members = lax.axis_size("dev")
    return lax.axis_index("grp"), lax.axis_index("dev"), members


def grp_at(grp, r):
    outer, inner = factors()
    return (grp // inner + r % outer) % outer * inner + (grp % inner + r // outer) % inner


def offset_of(grp, other):
    outer, inner = factors()
    return (other % inner - grp % inner + inner) % inner * outer + (
        other // inner - grp // inner + outer
    ) % outer


def negative(r):
    outer, inner = factors()
    return (-(r // outer)) % inner * outer + (-(r % outer)) % outer


def shift(value, axis, do, di, sizes):
    outer, inner = sizes
    pairs = [
        (((o + do) % outer) * inner + (i + di) % inner, o * inner + i)
        for o in range(outer)
        for i in range(inner)
    ]
    return lax.ppermute(value, axis, pairs)


def shift_grp(value, r):
    outer, _ = factors()
    return shift(value, "grp", r % outer, r // outer, factors())


def call(kernel, flops, outs, ins, scratch=(), aliases=None):
    specs = [SMEM_SPEC if scalar else VMEM_SPEC for _, scalar in ins]
    out_shape = tuple(jax.ShapeDtypeStruct(s, d) for s, d in outs)
    out_specs = tuple(
        SMEM_SPEC if len(s) == 1 and d == jnp.int32 else VMEM_SPEC for s, d in outs
    )
    moved = sum(x.size * x.dtype.itemsize for x, _ in ins)
    return pl.pallas_call(
        kernel,
        out_shape=out_shape,
        in_specs=specs,
        out_specs=out_specs,
        scratch_shapes=list(scratch),
        input_output_aliases=aliases or {},
        cost_estimate=pl.CostEstimate(
            flops=int(flops), bytes_accessed=int(moved), transcendentals=0
        ),
    )(*[x for x, _ in ins])


def split(value):
    high = value.astype(jnp.bfloat16)
    return high, (value - high.astype(jnp.float32)).astype(jnp.bfloat16)


def dot3(a, b, dims):
    one = functools.partial(
        lax.dot_general, dimension_numbers=dims, preferred_element_type=jnp.float32
    )
    return one(a[0], b[0]) + (one(a[0], b[1]) + one(a[1], b[0]))


def pick_kernel(blocks_dev, lists, sel, pair, tiles, near, far, rows, selm, count):
    grp, dev, members = place()
    device = grp * members + dev
    tile_dev, block_rows, _ = tiles.shape
    sel_dev = selm.shape[0]
    base = device * blocks_dev * block_rows
    lane = lax.broadcasted_iota(jnp.int32, (1, block_rows), 1)
    coded = jnp.zeros((1, block_rows), jnp.int32)
    for k in range(sel_dev):
        selm[k : k + 1, :] = (sel[k] - base) - lane
        coded = jnp.where(lane == k, pair[k], coded)
    near[...] = jnp.zeros_like(near)
    far[...] = jnp.zeros_like(far)
    for i in range(count.shape[0]):
        count[i] = 0
    offsets = selm[...]
    for t in range(tile_dev):
        row_block = lists[0, device * tile_dev + t] - device * blocks_dev
        hot = (offsets == row_block * block_rows).astype(jnp.bfloat16)
        rows[t] = jnp.dot(hot, tiles[t], preferred_element_type=jnp.float32).astype(jnp.bfloat16)
    high = coded // block_rows
    high_row = high.astype(jnp.float32).astype(jnp.bfloat16)
    low_row = (coded - high * block_rows).astype(jnp.float32).astype(jnp.bfloat16)
    for q in range(near.shape[0]):
        near[q, CAP, 0:1, :] = high_row
        near[q, CAP, 1:2, :] = low_row

    def step(t, carry):
        owner = lists[1, device * tile_dev + t] // blocks_dev
        rank = count[owner]
        count[owner] = rank + 1
        owner_grp = owner // members
        owner_dev = owner - owner_grp * members

        @pl.when((owner_grp == grp) & (owner_dev != dev))
        def _():
            near[owner_dev, rank] = rows[t]

        @pl.when(owner_grp != grp)
        def _():
            far[offset_of(grp, owner_grp), rank] = rows[t]

        return carry

    lax.fori_loop(0, tile_dev, step, 0)


def index_kernel(lists, sel, feats, blocks, own_feats, index):
    grp, dev, members = place()
    groups = lax.axis_size("grp")
    device = grp * members + dev
    blocks_dev, block_rows, _ = blocks.shape
    tile_dev = lists.shape[1] // (groups * members)
    sel_dev = own_feats.shape[0]
    base = device * blocks_dev * block_rows
    for c in range(blocks_dev):
        blocks[c] = feats[c * block_rows : (c + 1) * block_rows, :].astype(jnp.bfloat16)
    for k in range(sel_dev):
        own_feats[k : k + 1, :] = feats[pl.ds(sel[k] - base, 1), :]
    for i in range(index.shape[0]):
        index[i] = 0
    for q in range(members + groups):
        peer = grp * members + q if q < members else grp_at(grp, negative(q - members)) * members + dev

        def scan(t, hits, q=q, peer=peer):
            column = lists[1, peer * tile_dev + t]
            mine = column // blocks_dev == device
            index[q * (CAP + 1) + hits] = jnp.clip(column - device * blocks_dev, 0, blocks_dev - 1)
            return jnp.minimum(hits + mine.astype(jnp.int32), CAP)

        lax.fori_loop(0, tile_dev, scan, 0, unroll=4)


def partial_kernel(first, index, rows_in, blocks, part):
    for p in range(part.shape[0]):
        at = (first + p) * (CAP + 1)
        total = jnp.dot(rows_in[p, 0], blocks[index[at]], preferred_element_type=jnp.float32)
        for s in range(1, CAP):
            total += jnp.dot(
                rows_in[p, s], blocks[index[at + s]], preferred_element_type=jnp.float32
            )
        part[p] = total


def local_kernel(lists, own_feats, rows, blocks, local):
    grp, dev, members = place()
    device = grp * members + dev
    blocks_dev = blocks.shape[0]
    tile_dev = rows.shape[0]
    local[...] = own_feats[...]

    def add_tile(t, carry):
        column = lists[1, device * tile_dev + t]

        @pl.when(column // blocks_dev == device)
        def _():
            local[...] += jnp.dot(
                rows[t], blocks[column - device * blocks_dev], preferred_element_type=jnp.float32
            )

        return carry

    lax.fori_loop(0, tile_dev, add_tile, 0)


def combine_kernel(near_back, local, *rest):
    total = local[...]
    for p in range(near_back.shape[0]):
        total += near_back[p]
    for part in rest[:-1]:
        total += part[...]
    out = rest[-1]
    for p in range(out.shape[0]):
        out[p] = total


def split_kernel(value, high, mid):
    high[...], mid[...] = split(value[...])


def texts_kernel(*refs):
    pieces, (high, mid) = refs[:-2], refs[-2:]
    for r, piece in enumerate(pieces):
        rows = piece[...]
        norm = jnp.sqrt(jnp.sum(rows * rows, axis=1, keepdims=True) + EPS)
        high[r], mid[r] = split(rows / norm)


def forward_kernel(
    chosen, w_high, w_mid, t_high, t_mid, pair, ids, unit, slope, exps, row_total, sums
):
    grp, _, _ = place()
    groups = t_high.shape[0]
    before = dot3(split(chosen[...]), (w_high[...], w_mid[...]), PLAIN)
    bell = 0.5 * (1.0 + lax.erf(before * ROOT_HALF))
    hidden = before * bell
    norm = jnp.sqrt(jnp.sum(hidden * hidden, axis=1, keepdims=True) + EPS)
    nodes = hidden / norm
    unit[...] = nodes
    slope[...] = (bell + before * jnp.exp(-0.5 * before * before) * INV_ROOT_TWO_PI) / norm
    parts = split(nodes)
    rows = jnp.zeros((nodes.shape[0], 1), jnp.float32)
    positive = jnp.zeros((nodes.shape[0], 1), jnp.float32)
    for r in range(groups):
        scores = SCALE * dot3(parts, (t_high[r], t_mid[r]), BY_LAST)
        hit = pair[...] == ids[r]
        positive += jnp.sum(jnp.where(hit, scores, 0.0), axis=1, keepdims=True)
        grown = jnp.exp(scores)
        exps[r] = grown
        rows += jnp.sum(grown, axis=1, keepdims=True)
        sums[pl.ds(grp_at(grp, r), 1), :] = jnp.sum(grown, axis=0, keepdims=True)
    row_total[...] = rows
    lane = lax.broadcasted_iota(jnp.int32, (1, sums.shape[1]), 1)
    logs = jnp.sum(jnp.log(rows), axis=0, keepdims=True)
    found = jnp.sum(positive, axis=0, keepdims=True)
    sums[groups : groups + 1, :] = jnp.where(lane == 0, logs, jnp.where(lane == 1, found, 0.0))


def backward_kernel(
    exps, row_total, totals, pair, ids, t_high, t_mid, unit, slope, pre_grad, own_cols, loss
):
    grp, _, _ = place()
    groups = t_high.shape[0]
    sel_dev = own_cols.shape[2]
    row_share = 0.5 / row_total[...]
    node_dir = jnp.zeros(pre_grad.shape, jnp.float32)
    for r in range(groups):
        col_share = 0.5 / totals[pl.ds(grp_at(grp, r), 1), :]
        hit = (pair[...] == ids[r]).astype(jnp.float32)
        grads = exps[r] * (row_share + col_share) - hit
        own_cols[r] = grads[:, :sel_dev]
        node_dir += dot3(split(grads), (t_high[r], t_mid[r]), PLAIN)
    node_dir = SCALE * node_dir
    nodes = unit[...]
    along = jnp.sum(nodes * node_dir, axis=1, keepdims=True)
    pre_grad[...] = (node_dir - nodes * along) * slope[...]
    all_sel = groups * totals.shape[1]
    logs = totals[groups : groups + 1, 0:1] + jnp.sum(
        jnp.sum(jnp.log(totals[0:groups, :]), axis=1, keepdims=True), axis=0, keepdims=True
    )
    loss[...] = logs / (2.0 * all_sel) - totals[groups : groups + 1, 1:2] / all_sel


def rows_kernel(pre_grad, w_high, w_mid, near_grads, own_grads, own_half):
    _, dev, members = place()
    sel_dev = own_grads.shape[0]
    grads = dot3(split(pre_grad[...]), (w_high[...], w_mid[...]), BY_LAST)
    for q in range(members):
        part = grads[q * sel_dev : (q + 1) * sel_dev, :]
        near_grads[q] = part.astype(jnp.bfloat16)

        @pl.when(dev == q)
        def _(part=part):
            own_grads[...] = part
            own_half[...] = part.astype(jnp.bfloat16)


def text_part_kernel(own_cols, unit, part):
    parts = split(unit[...])
    for r in range(part.shape[0]):
        part[r] = SCALE * dot3(split(own_cols[r]), parts, BY_FIRST)


def text_end_kernel(texts, *rest):
    parts, out = rest[:-1], rest[-1]
    rows = texts[...]
    norm = jnp.sqrt(jnp.sum(rows * rows, axis=1, keepdims=True) + EPS)
    unit = rows / norm
    total = parts[0][...]
    for part in parts[1:]:
        total += part[...]
    out[...] = (total - unit * jnp.sum(unit * total, axis=1, keepdims=True)) / norm


def spread_kernel(lists, sel, index, near_in, rows, near_grads, own_grads, out):
    grp, dev, members = place()
    device = grp * members + dev
    tile_dev, sel_dev, block_rows = rows.shape
    blocks_dev = out.shape[0] // block_rows
    base = device * blocks_dev * block_rows
    out[...] = jnp.zeros_like(out)
    for q in range(members):
        for s in range(CAP):
            c = index[q * (CAP + 1) + s]
            span = pl.ds(pl.multiple_of(c * block_rows, block_rows), block_rows)
            out[span, :] += lax.dot_general(
                near_in[q, s], near_grads[q], BY_FIRST, preferred_element_type=jnp.float32
            )
    own = near_grads[dev]

    def add_tile(t, carry):
        column = lists[1, device * tile_dev + t]

        @pl.when(column // blocks_dev == device)
        def _():
            c = column - device * blocks_dev
            span = pl.ds(pl.multiple_of(c * block_rows, block_rows), block_rows)
            out[span, :] += lax.dot_general(
                rows[t], own, BY_FIRST, preferred_element_type=jnp.float32
            )

        return carry

    lax.fori_loop(0, tile_dev, add_tile, 0)
    for k in range(sel_dev):
        out[pl.ds(sel[k] - base, 1), :] += own_grads[k : k + 1, :]


def spread_far_kernel(first, index, so_far, *refs):
    out = refs[-1]
    count = (len(refs) - 1) // 2
    rows_in, grads = refs[:count], refs[count : 2 * count]
    block_rows = rows_in[0].shape[2]
    out[...] = so_far[...]
    for p in range(count):
        for s in range(CAP):
            c = index[(first + p) * (CAP + 1) + s]
            span = pl.ds(pl.multiple_of(c * block_rows, block_rows), block_rows)
            out[span, :] += lax.dot_general(
                rows_in[p][s], grads[p][...], BY_FIRST, preferred_element_type=jnp.float32
            )


def weight_kernel(*refs):
    out = refs[-1]
    rest = refs[:-1]
    total = None
    if len(rest) % 2:
        total, rest = rest[0][...], rest[1:]
    for i in range(0, len(rest), 2):
        term = dot3(split(rest[i][...]), split(rest[i + 1][...]), BY_FIRST)
        total = term if total is None else total + term
    out[...] = total


def shards(node_features, tiles, tile_list, weight, texts, selected, pairing):
    groups = lax.axis_size("grp")
    members = lax.axis_size("dev")
    grp_index = lax.axis_index("grp")
    dev_index = lax.axis_index("dev")
    block_rows = tiles.shape[1]
    width = node_features.shape[1]
    blocks_dev = node_features.shape[0] // block_rows
    tile_dev = tiles.shape[0]
    sel_dev = selected.shape[0]
    group_sel = sel_dev * members
    f32, half = jnp.float32, jnp.bfloat16
    outer, inner = factors()
    dev_outer, dev_inner = dev_factors()
    lists = tile_list.T
    dots = 2 * 3 * group_sel * width

    text_z = [texts] + [shift(texts, "dev", j, 0, dev_factors()) for j in range(1, dev_outer)]

    near_rows, far_rows, tile_rows = call(
        functools.partial(pick_kernel, blocks_dev),
        2 * tile_dev * sel_dev * block_rows * block_rows,
        [
            ((members, CAP + 1, sel_dev, block_rows), half),
            ((groups, CAP, sel_dev, block_rows), half),
            ((tile_dev, sel_dev, block_rows), half),
        ],
        [(lists, True), (selected, True), (pairing, True), (tiles, False)],
        [
            pltpu.VMEM((sel_dev, block_rows), jnp.int32),
            pltpu.SMEM((groups * members,), jnp.int32),
        ],
    )
    near_in = lax.all_to_all(near_rows, "dev", 0, 0, tiled=True)
    far_in = [shift_grp(far_rows[r], negative(r)) for r in range(1, groups)]

    blocks, own_feats, index = call(
        index_kernel,
        10**7,
        [
            ((blocks_dev, block_rows, width), half),
            ((sel_dev, width), f32),
            (((members + groups) * (CAP + 1),), jnp.int32),
        ],
        [(lists, True), (selected, True), (node_features, False)],
    )
    (near_part,) = call(
        functools.partial(partial_kernel, 0),
        2 * members * CAP * sel_dev * block_rows * width,
        [((members, sel_dev, width), f32)],
        [(index, True), (near_in, False), (blocks, False)],
    )
    near_back = lax.all_to_all(near_part, "dev", 0, 0, tiled=True)
    (far_part,) = call(
        functools.partial(partial_kernel, members + 1),
        2 * groups * CAP * sel_dev * block_rows * width,
        [((groups - 1, sel_dev, width), f32)],
        [(index, True), (jnp.stack(far_in), False), (blocks, False)],
    )
    far_back = [shift_grp(far_part[r - 1], r) for r in range(1, groups)]
    (local,) = call(
        local_kernel,
        2 * tile_dev * sel_dev * block_rows * width,
        [((sel_dev, width), f32)],
        [(lists, True), (own_feats, False), (tile_rows, False), (blocks, False)],
    )

    text_near = jnp.concatenate(text_z, axis=0)
    text_near = jnp.concatenate(
        [text_near] + [shift(text_near, "dev", 0, j, dev_factors()) for j in range(1, dev_inner)],
        axis=0,
    )
    text_pieces = gather_grp(text_near)
    t_high, t_mid = call(
        texts_kernel,
        10**8,
        [((groups, group_sel, width), half)] * 2,
        [(piece, False) for piece in text_pieces],
    )
    w_high, w_mid = call(split_kernel, 10**7, [((width, width), half)] * 2, [(weight, False)])
    dev_o = (dev_index // dev_inner + jnp.arange(dev_outer, dtype=jnp.int32)) % dev_outer
    dev_i = (dev_index % dev_inner + jnp.arange(dev_inner, dtype=jnp.int32)) % dev_inner
    dev_of = (dev_o[None, :] * dev_inner + dev_i[:, None]).reshape(-1)
    grp_of = grp_at(grp_index, jnp.arange(groups, dtype=jnp.int32))
    ids = (
        (grp_of[:, None, None] * members + dev_of[None, :, None]) * sel_dev
        + jnp.arange(sel_dev, dtype=jnp.int32)[None, None, :]
    ).reshape(groups, 1, group_sel)
    coded = near_in[:, CAP, :2, :sel_dev].astype(jnp.int32)
    pair = (coded[:, 0, :] * block_rows + coded[:, 1, :]).reshape(group_sel, 1)

    (copies,) = call(
        combine_kernel,
        10**6,
        [((members, sel_dev, width), f32)],
        [(near_back, False), (local, False)] + [(part, False) for part in far_back],
    )
    chosen = lax.all_to_all(copies, "dev", 0, 0, tiled=True).reshape(group_sel, width)
    chosen_pieces = gather_grp(chosen)

    unit, slope, exps, row_total, sums = call(
        forward_kernel,
        dots * (width + groups * group_sel),
        [
            ((group_sel, width), f32),
            ((group_sel, width), f32),
            ((groups, group_sel, group_sel), f32),
            ((group_sel, 1), f32),
            ((groups + 1, group_sel), f32),
        ],
        [(x, False) for x in (chosen, w_high, w_mid, t_high, t_mid, pair, ids)],
    )
    totals = lax.psum(sums, "grp")
    pre_grad, own_cols, loss = call(
        backward_kernel,
        dots * groups * group_sel,
        [
            ((group_sel, width), f32),
            ((groups, group_sel, sel_dev), f32),
            ((1, 1), f32),
        ],
        [(x, False) for x in (exps, row_total, totals, pair, ids, t_high, t_mid, unit, slope)],
    )
    pre_pieces = gather_grp(pre_grad)
    near_grads, own_grads, own_half = call(
        rows_kernel,
        dots * width,
        [((members, sel_dev, width), half), ((sel_dev, width), f32), ((sel_dev, width), half)],
        [(x, False) for x in (pre_grad, w_high, w_mid)],
    )
    far_grads = gather_grp(own_half)
    (text_part,) = call(
        text_part_kernel,
        2 * 3 * groups * sel_dev * group_sel * width,
        [((groups, sel_dev, width), f32)],
        [(own_cols, False), (unit, False)],
    )
    text_part = text_part.reshape(inner, outer, sel_dev, width)
    text_sum = text_part[0]
    for j in range(1, inner):
        text_sum = text_sum + shift_grp(text_part[j], negative(j * outer))
    text_terms = [text_sum[0]] + [
        shift_grp(text_sum[j], negative(j)) for j in range(1, outer)
    ]
    (grad_texts,) = call(
        text_end_kernel,
        10**6,
        [((sel_dev, width), f32)],
        [(texts, False)] + [(term, False) for term in text_terms],
    )
    (spread,) = call(
        spread_kernel,
        4 * tile_dev * sel_dev * block_rows * width,
        [(node_features.shape, f32)],
        [(x, True) for x in (lists, selected, index)]
        + [(x, False) for x in (near_in, tile_rows, near_grads, own_grads)],
    )
    (grad_nodes,) = call(
        functools.partial(spread_far_kernel, members + 1),
        4 * tile_dev * sel_dev * block_rows * width,
        [(node_features.shape, f32)],
        [(index, True), (spread, False)]
        + [(x, False) for x in far_in]
        + [(far_grads[negative(r)], False) for r in range(1, groups)],
        aliases={1: 0},
    )

    order = sorted(range(groups), key=lambda r: (r % outer > 0, r))
    grad_weight = None
    for r in order:
        ins = [(chosen_pieces[r], False), (pre_pieces[r], False)]
        first = [] if grad_weight is None else [(grad_weight, False)]
        (grad_weight,) = call(
            weight_kernel,
            dots * width,
            [((width, width), f32)],
            first + ins,
            aliases={0: 0} if first else None,
        )
    return (loss.reshape(()), grad_nodes, grad_weight, grad_texts)


def gather_grp(part):
    outer, inner = factors()
    pieces = [part] + [shift_grp(part, j) for j in range(1, outer)]
    return pieces + [shift_grp(p, j * outer) for j in range(1, inner) for p in pieces]


def solution(mesh):
    return jax.shard_map(
        shards,
        mesh=mesh,
        in_specs=(
            P(("grp", "dev"), None),
            P(("grp", "dev"), None, None),
            P(),
            P(),
            P(("grp", "dev"), None),
            P(("grp", "dev")),
            P(("grp", "dev")),
        ),
        out_specs=(P(), P(("grp", "dev"), None), P(), P(("grp", "dev"), None)),
        check_vma=False,
    )
```
